32 devices in a mesh: trans: 16 (over z, y, x), los: 2 (over core).
Axes of the slice: x: 2, y: 2, z: 4, core: 2. Of those that a mesh axis runs over, the one named last changes fastest.
Arguments:
- density: bfloat16 [2, 2048, 2048], P('los', 'trans'), may hold values from -6 to 6
- row_pos: float32 [2, 2048], replicated, may hold values from 0 to 2048
- col_pos: float32 [2, 2048], replicated, may hold values from 0 to 2048
- plane_of_slot: int32 [2], replicated, may hold values from 0 to 1, each once
- plane_bin: int32 [2], replicated, may hold values from 0 to 3, as said below
- efficiency: float32 [4, 2], replicated, may hold values from 0.3 to 3
Outputs:
- shear: float32 [2, 4, 2048, 2048], P(None, None, ('trans', 'los'))
The draws below stay inside these ranges and needn't reach their ends.
Inputs may be any that keep to these rules, and one draw needn't show every extreme that they name: `plane_bin`: some plane has bin 0 and some plane has bin 4 - 1.
All inputs are finite; a program needn't handle non-finite values.
Results may differ from the reference program's by a relative error of at most 0.006.
Values may be sent and summed in bfloat16 or wider, within the bound.
A program may use at most 64 MiB of HBM per device.

```python
import math
import jax
import jax.numpy as jnp
from jax import lax

GRID = 2048
MESH = 2048
BINS = 4
PLANES = 2


def positions_for(key, salt):
    scale_key = jax.random.fold_in(key, salt)
    offset_key = jax.random.fold_in(key, salt + 1)
    lower = 0.8
    scale = jax.random.uniform(scale_key, (PLANES, 1), jnp.float32, lower, 1.0)
    offset = jax.random.uniform(offset_key, (PLANES, 1), jnp.float32, 0.0, 1.0 * MESH)
    cells = jnp.arange(GRID, dtype=jnp.int32).astype(jnp.float32)
    return jnp.mod(offset + scale * cells[None, :], 1.0 * MESH).astype(jnp.float32)


def draw_row_pos(key, part):
    return positions_for(key, 31)


def draw_col_pos(key, part):
    return positions_for(key, 41)


def draw_plane_bin(key, part):
    first_key = jax.random.fold_in(key, 11)
    second_key = jax.random.fold_in(key, 12)
    drawn = jax.random.randint(first_key, (PLANES,), 0, BINS)
    forced = jax.random.randint(second_key, (), 0, PLANES)
    other = (forced + 1) % PLANES
    plane_index = jnp.arange(PLANES, dtype=jnp.int32)
    result = jnp.where(plane_index == forced, 0, drawn)
    result = jnp.where(plane_index == other, BINS - 1, result)
    return result.astype(jnp.int32)


def steps_of(own_key, extent, cuts, smallest, high):
    loudness, own = 1.0, jax.random.fold_in(own_key, 6)
    for dim, blocks in cuts:
        steps = jnp.exp(jax.random.uniform(jax.random.fold_in(own, dim), (blocks,), jnp.float32, smallest / len(cuts), high / len(cuts)))
        loudness = loudness * jnp.repeat(steps, extent[dim] // blocks).reshape([-1 if axis == dim else 1 for axis in range(len(extent))])
    return loudness


def noise(key, extent, width, limit, shards=(), held_as=jnp.bfloat16):
    level = steps_of(key, extent, shards, -0.22, 0.18) if shards else 1.0
    entries = jax.random.normal(key, extent, jnp.float32) * width * level
    return jnp.minimum(jnp.maximum(entries, -limit), limit).astype(held_as)


def setup_inputs(seed: int = 0) -> dict:
    streams_of = jax.random.split(jax.random.key(seed), 7)
    return {
        "density": noise(streams_of[0], (PLANES, MESH, MESH), 1.0, 6.0, ((0, 2), (1, 16))),
        "row_pos": draw_row_pos(jax.random.fold_in(streams_of[6], 71), 0),
        "col_pos": draw_col_pos(jax.random.fold_in(streams_of[6], 71), 0),
        "plane_of_slot": jax.random.permutation(streams_of[3], PLANES).astype(jnp.int32),
        "plane_bin": draw_plane_bin(jax.random.fold_in(streams_of[6], 71), 0),
        "efficiency": jnp.clip(jnp.exp(jax.random.uniform(streams_of[5], (BINS, PLANES), jnp.float32, math.log(0.3), math.log(3.0))), 0.3, 3.0),
    }


def hat_block(positions, mesh_cells):
    cells = jnp.arange(mesh_cells, dtype=jnp.int32).astype(jnp.float32)
    offset = positions[:, None] - cells[None, :] + 0.5 * mesh_cells
    folded = jnp.mod(offset, 1.0 * mesh_cells) - 0.5 * mesh_cells
    return jnp.maximum(1.0 - jnp.abs(folded), 0.0).astype(jnp.bfloat16)


def wave_numbers(length):
    index_all = jnp.arange(length, dtype=jnp.int32)
    return jnp.where(index_all < length // 2, index_all, index_all - length).astype(jnp.float32)


def shear_factors(wave_rows, wave_cols):
    square_sum = jnp.maximum(wave_rows * wave_rows + wave_cols * wave_cols, 1.0)
    return (wave_rows * wave_rows - wave_cols * wave_cols) / square_sum, 2.0 * wave_rows * wave_cols / square_sum


def reference(density, row_pos, col_pos, plane_of_slot, plane_bin, efficiency):
    planes_total = density.shape[0]
    mesh_cells = density.shape[2]
    bins_total = efficiency.shape[0]
    grid_cells = row_pos.shape[1]
    convergence = jnp.zeros((bins_total, grid_cells, grid_cells), jnp.float32)
    for slot_index in range(planes_total):
        plane_id = plane_of_slot[slot_index]
        row_weights = hat_block(row_pos[plane_id], mesh_cells)
        col_weights = hat_block(col_pos[plane_id], mesh_cells)
        half_product = jnp.dot(row_weights, density[slot_index], preferred_element_type=jnp.float32).astype(jnp.bfloat16)
        plane_map = jnp.dot(half_product, col_weights.T, preferred_element_type=jnp.float32)
        weights = efficiency[:, plane_id] * (jnp.arange(bins_total, dtype=jnp.int32) >= plane_bin[plane_id]).astype(jnp.float32)
        convergence = convergence + weights[:, None, None] * plane_map
    spectrum = jnp.fft.fft2(convergence)
    first_factor, second_factor = shear_factors(wave_numbers(grid_cells)[:, None], wave_numbers(grid_cells)[None, :])
    kernel = lax.complex(first_factor, second_factor)
    field = jnp.fft.ifft2(kernel[None] * spectrum)
    return jnp.stack([jnp.real(field), jnp.imag(field)]).astype(jnp.float32)
```

```python
import math

import jax
import jax.numpy as jnp
import numpy as np
from jax import lax
from jax.sharding import PartitionSpec as P

BF = jnp.bfloat16
F32 = jnp.float32
STEP = 32


def slot_layout(length, width):
    half = length // 2
    blocks = half // width
    block = np.arange(2 * half) // (2 * width)
    inner = np.arange(2 * half) % (2 * width)
    is_sine = inner >= width
    member = inner % width
    odd = block >= blocks // 2
    wave = 2 * (np.where(odd, block - blocks // 2, block) * width + member) + odd
    nyquist = is_sine & (wave == 0)
    wave = np.where(nyquist, half, wave)
    phase = np.where(is_sine & ~nyquist, 0.5 * np.pi, 0.0)
    return wave, phase


def small_tables(length, width):
    half = length // 2
    wave, phase = slot_layout(length, width)
    coarse = (np.arange(half // STEP)[:, None] * STEP * wave[None, :]) % length
    fine = (np.arange(STEP)[:, None] * wave[None, :]) % length
    coarse = coarse * (2 * np.pi / length)
    fine = fine * (2 * np.pi / length) + phase[None, :]
    return [np.float32(t) for t in (np.cos(coarse), np.sin(coarse), np.cos(fine), np.sin(fine))]


def full_table(length, width):
    half = length // 2
    cos_a, sin_a, cos_b, sin_b = [jnp.asarray(t) for t in small_tables(length, width)]
    table = cos_a[:, None] * cos_b[None] - sin_a[:, None] * sin_b[None]
    table = table.reshape(half, 2 * half).astype(BF)
    return table[:, :half], table[:, half:]


def hat_rows(positions, cells):
    base = jnp.floor(positions)
    frac = positions - base
    low = base.astype(jnp.int32) % cells
    high = (low + 1) % cells
    index = jnp.arange(cells, dtype=jnp.int32)[None, :]
    value = jnp.where(index == low[:, None], (1.0 - frac)[:, None], 0.0)
    return jnp.where(index == high[:, None], frac[:, None], value).astype(BF)


def dot(a, b, dims):
    return lax.dot_general(a, b, (dims, ((), ())), preferred_element_type=F32)


def lane_waves(length, width, index):
    blocks = length // 2 // width
    lane = lax.broadcasted_iota(jnp.int32, (1, 2 * width), 1)
    is_sine = lane >= width
    member = jnp.where(is_sine, lane - width, lane)
    odd = (index >= blocks // 2).astype(jnp.int32)
    wave = 2 * ((index - odd * (blocks // 2)) * width + member) + odd
    special = is_sine & (wave == 0)
    wave = jnp.where(special, -(length // 2), wave)
    return wave.astype(F32), special, is_sine


def body_plain(density, row_pos, col_pos, plane_of_slot, plane_bin, efficiency):
    count_trans = lax.axis_size("trans")
    count_los = lax.axis_size("los")
    cells = density.shape[2]
    length = row_pos.shape[1]
    half = length // 2
    width = half // count_trans
    planes = row_pos.shape[0]
    bins = efficiency.shape[0]
    rows_out = length // (count_trans * count_los)
    plane_id = plane_of_slot[lax.axis_index("los")]
    even, odd = full_table(length, width)

    cols_hat = hat_rows(col_pos[plane_id], cells)
    sampled = dot(density[0], cols_hat, ((1,), (1,)))
    plus = (sampled[:, :half] + sampled[:, half:]).astype(BF)
    minus = (sampled[:, :half] - sampled[:, half:]).astype(BF)
    spec = jnp.concatenate([dot(plus, even, ((1,), (0,))), dot(minus, odd, ((1,), (0,)))], axis=1).astype(BF)
    columns = lax.all_to_all(spec, "trans", split_axis=1, concat_axis=0, tiled=True)

    rows_hat = hat_rows(row_pos[plane_id], cells)
    mapped = dot(rows_hat, columns, ((1,), (0,)))
    plus = (mapped[:half] + mapped[half:]).astype(BF)
    minus = (mapped[:half] - mapped[half:]).astype(BF)
    freq = jnp.concatenate([dot(even, plus, ((0,), (0,))), dot(odd, minus, ((0,), (0,)))], axis=0)
    wave_np, phase_np = slot_layout(length, width)
    nyq_np = wave_np == half
    k1 = jnp.asarray(np.where(nyq_np, -half, wave_np), F32)[:, None]
    row_nyq = jnp.asarray(nyq_np)[:, None]
    row_sign = jnp.asarray(np.where(phase_np > 0, 1.0, -1.0), F32)[:, None]
    k2, lane_nyq, lane_sine = lane_waves(length, width, lax.axis_index("trans"))
    lane_sign = jnp.where(lane_sine, 1.0, -1.0)
    square = jnp.maximum(k1 * k1 + k2 * k2, 1.0)
    scale1 = jnp.asarray(np.where((wave_np == 0) | nyq_np, 1.0, 2.0) / length, F32)[:, None]
    scale2 = jnp.where((k2 == 0.0) | lane_nyq, 1.0, 2.0) / length
    scale = scale1 * scale2 / square
    d1 = (k1 * k1 - k2 * k2) * scale
    d2 = 2.0 * k1 * k2 * scale
    grid = freq.reshape(-1, 2, width, 2 * width)
    swap_rows = jnp.flip(grid, 1).reshape(freq.shape)
    swap_lanes = jnp.roll(freq, width, axis=1)
    swap_both = jnp.roll(swap_rows, width, axis=1)
    first = d1 * freq
    first = first + jnp.where(lane_nyq & ~row_nyq, row_sign * d2 * swap_rows, 0.0)
    first = first + jnp.where(row_nyq & ~lane_nyq, lane_sign * d2 * swap_lanes, 0.0)
    second = jnp.where(
        row_nyq,
        jnp.where(lane_nyq, d2 * freq, 0.0),
        jnp.where(lane_nyq, 0.0, -row_sign * lane_sign * d2 * swap_both),
    )
    fields = jnp.concatenate([first, second], axis=1).astype(BF)
    part_e = dot(even, fields[:half], ((1,), (0,)))
    part_o = dot(odd, fields[half:], ((1,), (0,)))
    back = jnp.concatenate([part_e + part_o, part_e - part_o], axis=0).astype(BF)

    back = back.reshape(count_trans * count_los, rows_out, 2, 2 * width)
    arrived = lax.all_to_all(back, ("trans", "los"), split_axis=0, concat_axis=0, tiled=True)
    arrived = arrived.reshape(count_trans, count_los, rows_out, 2, 2 * width).transpose(1, 3, 2, 0, 4)
    arrived = arrived.reshape(count_los * 2 * rows_out, length)
    part_e = dot(arrived[:, :half], even, ((1,), (1,)))
    part_o = dot(arrived[:, half:], odd, ((1,), (1,)))
    maps = jnp.concatenate([part_e + part_o, part_e - part_o], axis=1)
    maps = maps.reshape(count_los, 2, rows_out, length)
    slot_eff = efficiency[:, plane_of_slot]
    behind = jnp.arange(bins)[:, None] >= plane_bin[plane_of_slot][None, :]
    weights = jnp.where(behind, slot_eff, 0.0)
    total = 0.0
    for slot in range(planes):
        total = total + weights[None, :, slot, None, None] * maps[slot][:, None]
    return total


def solution(mesh):
    placed = (P("los", "trans", None), P(), P(), P(), P(), P())
    return jax.shard_map(
        body_plain,
        mesh=mesh,
        in_specs=placed,
        out_specs=P(None, None, ("trans", "los"), None),
        check_vma=False,
    )
```

```python
import functools

import jax
import jax.numpy as jnp
import numpy as np
from jax import lax
from jax.experimental import pallas as pl
from jax.experimental.pallas import tpu as pltpu
from jax.sharding import PartitionSpec as P

BF = jnp.bfloat16
F32 = jnp.float32
STEP = 32


def slot_layout(length, width):
    half = length // 2
    blocks = half // width
    block = np.arange(2 * half) // (2 * width)
    inner = np.arange(2 * half) % (2 * width)
    is_sine = inner >= width
    member = inner % width
    odd = block >= blocks // 2
    wave = 2 * (np.where(odd, block - blocks // 2, block) * width + member) + odd
    nyquist = is_sine & (wave == 0)
    wave = np.where(nyquist, half, wave)
    phase = np.where(is_sine & ~nyquist, 0.5 * np.pi, 0.0)
    return wave, phase


def small_tables(length, width):
    half = length // 2
    wave, phase = slot_layout(length, width)
    coarse = (np.arange(half // STEP)[:, None] * STEP * wave[None, :]) % length
    fine = (np.arange(STEP)[:, None] * wave[None, :]) % length
    coarse = coarse * (2 * np.pi / length)
    fine = fine * (2 * np.pi / length) + phase[None, :]
    return [np.float32(t) for t in (np.cos(coarse), np.sin(coarse), np.cos(fine), np.sin(fine))]


def full_table(length, width):
    half = length // 2
    cos_a, sin_a, cos_b, sin_b = [jnp.asarray(t) for t in small_tables(length, width)]
    table = cos_a[:, None] * cos_b[None] - sin_a[:, None] * sin_b[None]
    table = table.reshape(half, 2 * half).astype(BF)
    return table[:, :half], table[:, half:]


def hat_rows(positions, cells):
    base = jnp.floor(positions)
    frac = positions - base
    low = base.astype(jnp.int32) % cells
    high = (low + 1) % cells
    index = jnp.arange(cells, dtype=jnp.int32)[None, :]
    value = jnp.where(index == low[:, None], (1.0 - frac)[:, None], 0.0)
    return jnp.where(index == high[:, None], frac[:, None], value).astype(BF)


def dot(a, b, dims):
    return lax.dot_general(a, b, (dims, ((), ())), preferred_element_type=F32)


def lane_waves(length, width, index):
    blocks = length // 2 // width
    lane = lax.broadcasted_iota(jnp.int32, (1, 2 * width), 1)
    is_sine = lane >= width
    member = jnp.where(is_sine, lane - width, lane)
    odd = (index >= blocks // 2).astype(jnp.int32)
    wave = 2 * ((index - odd * (blocks // 2)) * width + member) + odd
    special = is_sine & (wave == 0)
    wave = jnp.where(special, -(length // 2), wave)
    return wave.astype(F32), special, is_sine


def body_plain(density, row_pos, col_pos, plane_of_slot, plane_bin, efficiency):
    count_trans = lax.axis_size("trans")
    count_los = lax.axis_size("los")
    cells = density.shape[2]
    length = row_pos.shape[1]
    half = length // 2
    width = half // count_trans
    planes = row_pos.shape[0]
    bins = efficiency.shape[0]
    rows_out = length // (count_trans * count_los)
    plane_id = plane_of_slot[lax.axis_index("los")]
    even, odd = full_table(length, width)

    cols_hat = hat_rows(col_pos[plane_id], cells)
    sampled = dot(density[0], cols_hat, ((1,), (1,)))
    plus = (sampled[:, :half] + sampled[:, half:]).astype(BF)
    minus = (sampled[:, :half] - sampled[:, half:]).astype(BF)
    spec = jnp.concatenate([dot(plus, even, ((1,), (0,))), dot(minus, odd, ((1,), (0,)))], axis=1).astype(BF)
    columns = lax.all_to_all(spec, "trans", split_axis=1, concat_axis=0, tiled=True)

    rows_hat = hat_rows(row_pos[plane_id], cells)
    mapped = dot(rows_hat, columns, ((1,), (0,)))
    plus = (mapped[:half] + mapped[half:]).astype(BF)
    minus = (mapped[:half] - mapped[half:]).astype(BF)
    freq = jnp.concatenate([dot(even, plus, ((0,), (0,))), dot(odd, minus, ((0,), (0,)))], axis=0)
    wave_np, phase_np = slot_layout(length, width)
    nyq_np = wave_np == half
    k1 = jnp.asarray(np.where(nyq_np, -half, wave_np), F32)[:, None]
    row_nyq = jnp.asarray(nyq_np)[:, None]
    row_sign = jnp.asarray(np.where(phase_np > 0, 1.0, -1.0), F32)[:, None]
    k2, lane_nyq, lane_sine = lane_waves(length, width, lax.axis_index("trans"))
    lane_sign = jnp.where(lane_sine, 1.0, -1.0)
    square = jnp.maximum(k1 * k1 + k2 * k2, 1.0)
    scale1 = jnp.asarray(np.where((wave_np == 0) | nyq_np, 1.0, 2.0) / length, F32)[:, None]
    scale2 = jnp.where((k2 == 0.0) | lane_nyq, 1.0, 2.0) / length
    scale = scale1 * scale2 / square
    d1 = (k1 * k1 - k2 * k2) * scale
    d2 = 2.0 * k1 * k2 * scale
    grid = freq.reshape(-1, 2, width, 2 * width)
    swap_rows = jnp.flip(grid, 1).reshape(freq.shape)
    swap_lanes = jnp.roll(freq, width, axis=1)
    swap_both = jnp.roll(swap_rows, width, axis=1)
    first = d1 * freq
    first = first + jnp.where(lane_nyq & ~row_nyq, row_sign * d2 * swap_rows, 0.0)
    first = first + jnp.where(row_nyq & ~lane_nyq, lane_sign * d2 * swap_lanes, 0.0)
    second = jnp.where(
        row_nyq,
        jnp.where(lane_nyq, d2 * freq, 0.0),
        jnp.where(lane_nyq, 0.0, -row_sign * lane_sign * d2 * swap_both),
    )
    fields = jnp.concatenate([first, second], axis=1).astype(BF)
    part_e = dot(even, fields[:half], ((1,), (0,)))
    part_o = dot(odd, fields[half:], ((1,), (0,)))
    back = jnp.concatenate([part_e + part_o, part_e - part_o], axis=0).astype(BF)

    back = back.reshape(count_trans * count_los, rows_out, 2, 2 * width)
    arrived = lax.all_to_all(back, ("trans", "los"), split_axis=0, concat_axis=0, tiled=True)
    arrived = arrived.reshape(count_trans, count_los, rows_out, 2, 2 * width).transpose(1, 3, 2, 0, 4)
    arrived = arrived.reshape(count_los * 2 * rows_out, length)
    part_e = dot(arrived[:, :half], even, ((1,), (1,)))
    part_o = dot(arrived[:, half:], odd, ((1,), (1,)))
    maps = jnp.concatenate([part_e + part_o, part_e - part_o], axis=1)
    maps = maps.reshape(count_los, 2, rows_out, length)
    slot_eff = efficiency[:, plane_of_slot]
    behind = jnp.arange(bins)[:, None] >= plane_bin[plane_of_slot][None, :]
    weights = jnp.where(behind, slot_eff, 0.0)
    total = 0.0
    for slot in range(planes):
        total = total + weights[None, :, slot, None, None] * maps[slot][:, None]
    return total


def fold_waves(length, width, block, inner):
    blocks = length // 2 // width
    is_sine = inner >= width
    member = jnp.where(is_sine, inner - width, inner)
    odd = (block >= blocks // 2).astype(jnp.int32)
    wave = 2 * ((block - odd * (blocks // 2)) * width + member) + odd
    nyquist = is_sine & (wave == 0)
    ends = (wave == 0) & ((block == 0) | ~is_sine)
    wave = jnp.where(nyquist, -(length // 2), wave)
    return wave.astype(F32), nyquist, is_sine, ends


def fill_hat(out_ref, low_ref, frac_ref, positions_on_lanes):
    cells = out_ref.shape[0]
    part = 128

    def step(i, carry):
        rows = pl.ds(pl.multiple_of(i * part, part), part)
        shape = (part, out_ref.shape[1])
        if positions_on_lanes:
            low, frac = low_ref[...], frac_ref[...]
            index = lax.broadcasted_iota(jnp.int32, shape, 0) + i * part
        else:
            low, frac = low_ref[rows, :], frac_ref[rows, :]
            index = lax.broadcasted_iota(jnp.int32, shape, 1)
        high = jnp.where(low == cells - 1, 0, low + 1)
        value = jnp.where(index == high, frac, 0.0)
        value = jnp.where(index == low, 1.0 - frac, value)
        out_ref[rows, :] = value.astype(BF)
        return carry

    lax.fori_loop(0, cells // part, step, 0)


def middle_kernel(
    count_trans, count_los, length,
    dens_ref, clow_ref, cfrac_ref, rlow_ref, rfrac_ref, cos_a, sin_a, cos_b, sin_b,
    out_ref, table_out,
    table, hat, halves, send1, recv1, turned, fields, send2,
    ssem1, rsem1, ssem2, rsem2, lsem,
):
    me_t = lax.axis_index("trans")
    me_l = lax.axis_index("los")
    devices = count_trans * count_los
    me = me_t * count_los + me_l
    half = length // 2
    width = half // count_trans
    lanes = 2 * width
    rows_out = length // devices
    chunk = 256
    barrier = pltpu.get_barrier_semaphore()

    def greet(i, carry):
        other = lax.rem(me + i, devices)
        pl.semaphore_signal(
            barrier, inc=1,
            device_id=(other // count_los, lax.rem(other, count_los)),
            device_id_type=pl.DeviceIdType.MESH,
        )
        return carry

    lax.fori_loop(1, devices, greet, 0)

    def table_step(i, carry):
        rows = pl.ds(pl.multiple_of(i * STEP, STEP), STEP)
        value = cos_a[pl.ds(i, 1), :] * cos_b[...] - sin_a[pl.ds(i, 1), :] * sin_b[...]
        table[rows, :] = value.astype(BF)
        return carry

    lax.fori_loop(0, half // STEP, table_step, 0)
    table_copy = pltpu.make_async_copy(table, table_out, lsem.at[0])
    table_copy.start()

    fill_hat(hat, clow_ref, cfrac_ref, True)
    for c in range(half // chunk):
        low = jnp.dot(dens_ref[...], hat[:, c * chunk : (c + 1) * chunk], preferred_element_type=F32)
        high = jnp.dot(
            dens_ref[...], hat[:, half + c * chunk : half + (c + 1) * chunk],
            preferred_element_type=F32,
        )
        halves[0, :, c * chunk : (c + 1) * chunk] = (low + high).astype(BF)
        halves[1, :, c * chunk : (c + 1) * chunk] = (low - high).astype(BF)
    for c in range(length // chunk):
        spec = jnp.dot(
            halves[c * chunk // half], table[:, c * chunk : (c + 1) * chunk],
            preferred_element_type=F32,
        ).astype(BF)
        for k in range(chunk // lanes):
            send1[c * (chunk // lanes) + k] = spec[:, k * lanes : (k + 1) * lanes]

    pl.semaphore_wait(barrier, devices - 1)

    def copy1(target, source):
        return pltpu.make_async_remote_copy(
            src_ref=send1.at[target], dst_ref=recv1.at[source],
            send_sem=ssem1.at[target], recv_sem=rsem1.at[source],
            device_id=(target, me_l), device_id_type=pl.DeviceIdType.MESH,
        )

    def start1(i, carry):
        copy1(lax.rem(me_t + i, count_trans), me_t).start()
        return carry

    lax.fori_loop(1, count_trans, start1, 0)
    own1 = pltpu.make_async_copy(send1.at[me_t], recv1.at[me_t], lsem.at[1])
    own1.start()
    fill_hat(hat, rlow_ref, rfrac_ref, False)
    own1.wait()

    def wait1(i, carry):
        other = lax.rem(me_t + i, count_trans)
        copy1(other, me_t).wait_send()
        copy1(me_t, other).wait_recv()
        return carry

    lax.fori_loop(1, count_trans, wait1, 0)

    columns = recv1[...].reshape(hat.shape[1], lanes)
    for c in range(half // chunk):
        low = jnp.dot(hat[c * chunk : (c + 1) * chunk, :], columns, preferred_element_type=F32)
        high = jnp.dot(
            hat[half + c * chunk : half + (c + 1) * chunk, :], columns,
            preferred_element_type=F32,
        )
        turned[0, :, c * chunk : (c + 1) * chunk] = (low + high).T.astype(BF)
        turned[1, :, c * chunk : (c + 1) * chunk] = (low - high).T.astype(BF)

    shape = (lanes, lanes)
    k2, lane_nyq, lane_sine, lane_end = fold_waves(
        length, width, me_t, lax.broadcasted_iota(jnp.int32, shape, 0)
    )
    lane_sign = jnp.where(lane_sine, 1.0, -1.0)
    scale2 = jnp.where(lane_end | lane_nyq, 1.0, 2.0) * (1.0 / length)
    inner = lax.broadcasted_iota(jnp.int32, shape, 1)
    for c in range(length // chunk):
        freq2 = jnp.dot(
            turned[c * chunk // half], table[:, c * chunk : (c + 1) * chunk],
            preferred_element_type=F32,
        )
        for k in range(chunk // lanes):
            block = c * (chunk // lanes) + k
            freq = freq2[:, k * lanes : (k + 1) * lanes]
            k1, row_nyq, row_sine, row_end = fold_waves(length, width, jnp.int32(block), inner)
            row_sign = jnp.where(row_sine, 1.0, -1.0)
            scale1 = jnp.where(row_end | row_nyq, 1.0, 2.0) * (1.0 / length)
            scale = scale1 * scale2 / jnp.maximum(k1 * k1 + k2 * k2, 1.0)
            d1 = (k1 * k1 - k2 * k2) * scale
            d2 = 2.0 * k1 * k2 * scale
            swap_rows = pltpu.roll(freq, width, 1)
            swap_lanes = jnp.concatenate([freq[width:], freq[:width]], axis=0)
            swap_both = pltpu.roll(swap_lanes, width, 1)
            first = d1 * freq
            extra = jnp.where(lane_nyq, row_sign * d2 * swap_rows, 0.0)
            second = jnp.where(lane_nyq, 0.0, -row_sign * lane_sign * d2 * swap_both)
            if block == 0:
                extra = jnp.where(
                    row_nyq, jnp.where(lane_nyq, 0.0, lane_sign * d2 * swap_lanes), extra
                )
                second = jnp.where(row_nyq, jnp.where(lane_nyq, d2 * freq, 0.0), second)
            where = slice(block * lanes, (block + 1) * lanes)
            fields[:lanes, where] = (first + extra).astype(BF)
            fields[lanes:, where] = second.astype(BF)

    contract = (((1,), (1,)), ((), ()))
    per = chunk // rows_out
    for c in range(half // chunk):
        rows = slice(c * chunk, (c + 1) * chunk)
        part_e = lax.dot_general(
            table[rows, :half], fields[:, :half], contract, preferred_element_type=F32
        )
        part_o = lax.dot_general(
            table[rows, half:], fields[:, half:], contract, preferred_element_type=F32
        )
        for offset, value in ((0, part_e + part_o), (devices // 2, part_e - part_o)):
            value = value.astype(BF)
            for k in range(per):
                for comp in range(2):
                    send2[offset + c * per + k, comp] = value[
                        k * rows_out : (k + 1) * rows_out, comp * lanes : (comp + 1) * lanes
                    ]

    def place(other):
        begin = pl.multiple_of((other // count_los) * lanes, lanes)
        return out_ref.at[lax.rem(other, count_los), :, :, pl.ds(begin, lanes)]

    def copy2(target, source):
        return pltpu.make_async_remote_copy(
            src_ref=send2.at[target], dst_ref=place(source),
            send_sem=ssem2.at[target], recv_sem=rsem2.at[source],
            device_id=(target // count_los, lax.rem(target, count_los)),
            device_id_type=pl.DeviceIdType.MESH,
        )

    def start2(i, carry):
        copy2(lax.rem(me + i, devices), me).start()
        return carry

    lax.fori_loop(1, devices, start2, 0)
    own2 = pltpu.make_async_copy(send2.at[me], place(me), lsem.at[2])
    own2.start()
    own2.wait()

    def wait2(i, carry):
        other = lax.rem(me + i, devices)
        copy2(other, me).wait_send()
        copy2(me, other).wait_recv()
        return carry

    lax.fori_loop(1, devices, wait2, 0)
    table_copy.wait()


def body_kernel(density, row_pos, col_pos, plane_of_slot, plane_bin, efficiency):
    count_trans = lax.axis_size("trans")
    count_los = lax.axis_size("los")
    rows_in, cells = density.shape[1:]
    length = row_pos.shape[1]
    half = length // 2
    width = half // count_trans
    lanes = 2 * width
    planes = row_pos.shape[0]
    bins = efficiency.shape[0]
    devices = count_trans * count_los
    rows_out = length // devices

    slots = jnp.arange(planes, dtype=jnp.int32)
    plane_id = jnp.sum(jnp.where(slots == lax.axis_index("los"), plane_of_slot, 0))

    def split(positions):
        here = jnp.sum(jnp.where((slots == plane_id)[:, None], positions, 0.0), axis=0)
        base = jnp.floor(here)
        low = base.astype(jnp.int32)
        return jnp.where(low >= cells, low - cells, low), here - base

    clow, cfrac = split(col_pos)
    rlow, rfrac = split(row_pos)
    tables = [jnp.asarray(t) for t in small_tables(length, width)]
    vmem = pl.BlockSpec(memory_space=pltpu.VMEM)
    arrived, table = pl.pallas_call(
        functools.partial(middle_kernel, count_trans, count_los, length),
        out_shape=[
            jax.ShapeDtypeStruct((count_los, 2, rows_out, length), BF),
            jax.ShapeDtypeStruct((half, length), BF),
        ],
        in_specs=[vmem] * 9,
        out_specs=[vmem, pl.BlockSpec(memory_space=pl.ANY)],
        scratch_shapes=[
            pltpu.VMEM((half, length), BF),
            pltpu.VMEM((length, cells), BF),
            pltpu.VMEM((2, rows_in, half), BF),
            pltpu.VMEM((count_trans, rows_in, lanes), BF),
            pltpu.VMEM((count_trans, rows_in, lanes), BF),
            pltpu.VMEM((2, lanes, half), BF),
            pltpu.VMEM((2 * lanes, length), BF),
            pltpu.VMEM((devices, 2, rows_out, lanes), BF),
            pltpu.SemaphoreType.DMA((count_trans,)),
            pltpu.SemaphoreType.DMA((count_trans,)),
            pltpu.SemaphoreType.DMA((devices,)),
            pltpu.SemaphoreType.DMA((devices,)),
            pltpu.SemaphoreType.DMA((3,)),
        ],
        compiler_params=pltpu.CompilerParams(
            collective_id=0, has_side_effects=True, vmem_limit_bytes=56 * 1024 * 1024
        ),
    )(
        density[0], clow[None, :], cfrac[None, :], rlow[:, None], rfrac[:, None], *tables
    )
    arrived = arrived.reshape(count_los * 2 * rows_out, length)
    part_e = dot(arrived[:, :half], table[:, :half], ((1,), (1,)))
    part_o = dot(arrived[:, half:], table[:, half:], ((1,), (1,)))
    maps = jnp.concatenate([part_e + part_o, part_e - part_o], axis=1)
    maps = maps.reshape(count_los, 2, rows_out, length)
    total = 0.0
    for slot in range(planes):
        chosen = slots == plane_of_slot[slot]
        slot_eff = jnp.sum(jnp.where(chosen[None, :], efficiency, 0.0), axis=1)
        first_bin = jnp.sum(jnp.where(chosen, plane_bin, 0))
        weight = jnp.where(jnp.arange(bins) >= first_bin, slot_eff, 0.0)
        total = total + weight[None, :, None, None] * maps[slot][:, None]
    return total


def body(density, row_pos, *rest):
    length = row_pos.shape[1]
    fits = length // lax.axis_size("trans") == 128 and density.shape[1] == 128
    fits = fits and length % 512 == 0 and density.shape[2] == length
    return (body_kernel if fits else body_plain)(density, row_pos, *rest)


def solution(mesh):
    placed = (P("los", "trans", None), P(), P(), P(), P(), P())
    return jax.shard_map(
        body,
        mesh=mesh,
        in_specs=placed,
        out_specs=P(None, None, ("trans", "los"), None),
        check_vma=False,
    )
```

```python
import functools

import jax
import jax.numpy as jnp
import numpy as np
from jax import lax
from jax.experimental import pallas as pl
from jax.experimental.pallas import tpu as pltpu
from jax.sharding import PartitionSpec as P

BF = jnp.bfloat16
F32 = jnp.float32
STEP = 32


def slot_layout(length, width):
    half = length // 2
    blocks = half // width
    block = np.arange(2 * half) // (2 * width)
    inner = np.arange(2 * half) % (2 * width)
    is_sine = inner >= width
    member = inner % width
    odd = block >= blocks // 2
    wave = 2 * (np.where(odd, block - blocks // 2, block) * width + member) + odd
    nyquist = is_sine & (wave == 0)
    wave = np.where(nyquist, half, wave)
    phase = np.where(is_sine & ~nyquist, 0.5 * np.pi, 0.0)
    return wave, phase


def small_tables(length, width):
    half = length // 2
    wave, phase = slot_layout(length, width)
    coarse = (np.arange(half // STEP)[:, None] * STEP * wave[None, :]) % length
    fine = (np.arange(STEP)[:, None] * wave[None, :]) % length
    coarse = coarse * (2 * np.pi / length)
    fine = fine * (2 * np.pi / length) + phase[None, :]
    return [np.float32(t) for t in (np.cos(coarse), np.sin(coarse), np.cos(fine), np.sin(fine))]


def full_table(length, width):
    half = length // 2
    cos_a, sin_a, cos_b, sin_b = [jnp.asarray(t) for t in small_tables(length, width)]
    table = cos_a[:, None] * cos_b[None] - sin_a[:, None] * sin_b[None]
    table = table.reshape(half, 2 * half).astype(BF)
    return table[:, :half], table[:, half:]


def hat_rows(positions, cells):
    base = jnp.floor(positions)
    frac = positions - base
    low = base.astype(jnp.int32) % cells
    high = (low + 1) % cells
    index = jnp.arange(cells, dtype=jnp.int32)[None, :]
    value = jnp.where(index == low[:, None], (1.0 - frac)[:, None], 0.0)
    return jnp.where(index == high[:, None], frac[:, None], value).astype(BF)


def dot(a, b, dims):
    return lax.dot_general(a, b, (dims, ((), ())), preferred_element_type=F32)


def lane_waves(length, width, index):
    blocks = length // 2 // width
    lane = lax.broadcasted_iota(jnp.int32, (1, 2 * width), 1)
    is_sine = lane >= width
    member = jnp.where(is_sine, lane - width, lane)
    odd = (index >= blocks // 2).astype(jnp.int32)
    wave = 2 * ((index - odd * (blocks // 2)) * width + member) + odd
    special = is_sine & (wave == 0)
    wave = jnp.where(special, -(length // 2), wave)
    return wave.astype(F32), special, is_sine


def body_plain(density, row_pos, col_pos, plane_of_slot, plane_bin, efficiency):
    count_trans = lax.axis_size("trans")
    count_los = lax.axis_size("los")
    cells = density.shape[2]
    length = row_pos.shape[1]
    half = length // 2
    width = half // count_trans
    planes = row_pos.shape[0]
    bins = efficiency.shape[0]
    rows_out = length // (count_trans * count_los)
    plane_id = plane_of_slot[lax.axis_index("los")]
    even, odd = full_table(length, width)

    cols_hat = hat_rows(col_pos[plane_id], cells)
    sampled = dot(density[0], cols_hat, ((1,), (1,)))
    plus = (sampled[:, :half] + sampled[:, half:]).astype(BF)
    minus = (sampled[:, :half] - sampled[:, half:]).astype(BF)
    spec = jnp.concatenate([dot(plus, even, ((1,), (0,))), dot(minus, odd, ((1,), (0,)))], axis=1).astype(BF)
    columns = lax.all_to_all(spec, "trans", split_axis=1, concat_axis=0, tiled=True)

    rows_hat = hat_rows(row_pos[plane_id], cells)
    mapped = dot(rows_hat, columns, ((1,), (0,)))
    plus = (mapped[:half] + mapped[half:]).astype(BF)
    minus = (mapped[:half] - mapped[half:]).astype(BF)
    freq = jnp.concatenate([dot(even, plus, ((0,), (0,))), dot(odd, minus, ((0,), (0,)))], axis=0)
    wave_np, phase_np = slot_layout(length, width)
    nyq_np = wave_np == half
    k1 = jnp.asarray(np.where(nyq_np, -half, wave_np), F32)[:, None]
    row_nyq = jnp.asarray(nyq_np)[:, None]
    row_sign = jnp.asarray(np.where(phase_np > 0, 1.0, -1.0), F32)[:, None]
    k2, lane_nyq, lane_sine = lane_waves(length, width, lax.axis_index("trans"))
    lane_sign = jnp.where(lane_sine, 1.0, -1.0)
    square = jnp.maximum(k1 * k1 + k2 * k2, 1.0)
    scale1 = jnp.asarray(np.where((wave_np == 0) | nyq_np, 1.0, 2.0) / length, F32)[:, None]
    scale2 = jnp.where((k2 == 0.0) | lane_nyq, 1.0, 2.0) / length
    scale = scale1 * scale2 / square
    d1 = (k1 * k1 - k2 * k2) * scale
    d2 = 2.0 * k1 * k2 * scale
    grid = freq.reshape(-1, 2, width, 2 * width)
    swap_rows = jnp.flip(grid, 1).reshape(freq.shape)
    swap_lanes = jnp.roll(freq, width, axis=1)
    swap_both = jnp.roll(swap_rows, width, axis=1)
    first = d1 * freq
    first = first + jnp.where(lane_nyq & ~row_nyq, row_sign * d2 * swap_rows, 0.0)
    first = first + jnp.where(row_nyq & ~lane_nyq, lane_sign * d2 * swap_lanes, 0.0)
    second = jnp.where(
        row_nyq,
        jnp.where(lane_nyq, d2 * freq, 0.0),
        jnp.where(lane_nyq, 0.0, -row_sign * lane_sign * d2 * swap_both),
    )
    fields = jnp.concatenate([first, second], axis=1).astype(BF)
    part_e = dot(even, fields[:half], ((1,), (0,)))
    part_o = dot(odd, fields[half:], ((1,), (0,)))
    back = jnp.concatenate([part_e + part_o, part_e - part_o], axis=0).astype(BF)

    back = back.reshape(count_trans * count_los, rows_out, 2, 2 * width)
    arrived = lax.all_to_all(back, ("trans", "los"), split_axis=0, concat_axis=0, tiled=True)
    arrived = arrived.reshape(count_trans, count_los, rows_out, 2, 2 * width).transpose(1, 3, 2, 0, 4)
    arrived = arrived.reshape(count_los * 2 * rows_out, length)
    part_e = dot(arrived[:, :half], even, ((1,), (1,)))
    part_o = dot(arrived[:, half:], odd, ((1,), (1,)))
    maps = jnp.concatenate([part_e + part_o, part_e - part_o], axis=1)
    maps = maps.reshape(count_los, 2, rows_out, length)
    slot_eff = efficiency[:, plane_of_slot]
    behind = jnp.arange(bins)[:, None] >= plane_bin[plane_of_slot][None, :]
    weights = jnp.where(behind, slot_eff, 0.0)
    total = 0.0
    for slot in range(planes):
        total = total + weights[None, :, slot, None, None] * maps[slot][:, None]
    return total


def fold_waves(length, width, block, inner):
    blocks = length // 2 // width
    is_sine = inner >= width
    member = jnp.where(is_sine, inner - width, inner)
    odd = (block >= blocks // 2).astype(jnp.int32)
    wave = 2 * ((block - odd * (blocks // 2)) * width + member) + odd
    nyquist = is_sine & (wave == 0)
    ends = (wave == 0) & ((block == 0) | ~is_sine)
    wave = jnp.where(nyquist, -(length // 2), wave)
    return wave.astype(F32), nyquist, is_sine, ends


def split_positions(spot, pos_ref, plane_id, cells):
    here = pos_ref[0:1, :]
    for plane in range(1, pos_ref.shape[0]):
        here = jnp.where(plane_id == plane, pos_ref[plane : plane + 1, :], here)
    base = jnp.floor(here)
    low = jnp.where(base >= cells, base - cells, base)
    spot[0:1, :] = low
    spot[1:2, :] = jnp.where(low == cells - 1, 0.0, low + 1.0)
    spot[2:3, :] = here - base


def fill_hat(out_ref, spot, positions_on_lanes):
    cells = out_ref.shape[0]
    part = 128

    def step(i, carry):
        rows = pl.ds(pl.multiple_of(i * part, part), part)
        if not positions_on_lanes:
            low, high, frac = [
                jnp.broadcast_to(spot[k : k + 1, rows], (part, part)).T for k in range(3)
            ]
            less = 1.0 - frac
        for j in range(out_ref.shape[1] // part):
            columns = slice(j * part, (j + 1) * part)
            if positions_on_lanes:
                low, high, frac = [spot[k : k + 1, columns] for k in range(3)]
                less = 1.0 - frac
                index = lax.broadcasted_iota(jnp.int32, (part, part), 0) + i * part
            else:
                index = lax.broadcasted_iota(jnp.int32, (part, part), 1) + j * part
            index = index.astype(F32)
            value = jnp.where(index == high, frac, 0.0)
            value = jnp.where(index == low, less, value)
            out_ref[rows, columns] = value.astype(BF)
        return carry

    lax.fori_loop(0, cells // part, step, 0)


def middle_kernel(
    count_trans, count_los, length,
    slot_ref, dens_ref, row_ref, col_ref, cos_a, sin_a, cos_b, sin_b,
    out_ref, table_out,
    table, hat, halves, send1, recv1, turned, fields, send2, spot,
    ssem1, rsem1, ssem2, rsem2, lsem,
):
    me_t = lax.axis_index("trans")
    me_l = lax.axis_index("los")
    devices = count_trans * count_los
    me = me_t * count_los + me_l
    half = length // 2
    width = half // count_trans
    lanes = 2 * width
    rows_out = length // devices
    chunk = 256
    barrier = pltpu.get_barrier_semaphore()

    def greet(i, carry):
        other = lax.rem(me + i, devices)
        pl.semaphore_signal(
            barrier, inc=1,
            device_id=(other // count_los, lax.rem(other, count_los)),
            device_id_type=pl.DeviceIdType.MESH,
        )
        return carry

    lax.fori_loop(1, devices, greet, 0)

    def table_step(i, carry):
        rows = pl.ds(pl.multiple_of(i * STEP, STEP), STEP)
        value = cos_a[pl.ds(i, 1), :] * cos_b[...] - sin_a[pl.ds(i, 1), :] * sin_b[...]
        table[rows, :] = value.astype(BF)
        return carry

    lax.fori_loop(0, half // STEP, table_step, 0)
    table_copy = pltpu.make_async_copy(table, table_out, lsem.at[0])
    table_copy.start()

    plane_id = slot_ref[me_l]
    split_positions(spot, col_ref, plane_id, hat.shape[0])
    fill_hat(hat, spot, True)
    for c in range(half // chunk):
        low = jnp.dot(dens_ref[...], hat[:, c * chunk : (c + 1) * chunk], preferred_element_type=F32)
        high = jnp.dot(
            dens_ref[...], hat[:, half + c * chunk : half + (c + 1) * chunk],
            preferred_element_type=F32,
        )
        halves[0, :, c * chunk : (c + 1) * chunk] = (low + high).astype(BF)
        halves[1, :, c * chunk : (c + 1) * chunk] = (low - high).astype(BF)
    def copy1(target, source):
        return pltpu.make_async_remote_copy(
            src_ref=send1.at[target], dst_ref=recv1.at[source],
            send_sem=ssem1.at[target], recv_sem=rsem1.at[source],
            device_id=(target, me_l), device_id_type=pl.DeviceIdType.MESH,
        )

    pl.semaphore_wait(barrier, devices - 1)
    chunks1 = length // chunk
    per1 = chunk // lanes

    def spectrum_step(i, carry):
        c = lax.rem(me_t // per1 + chunks1 // 2 + i, chunks1)
        columns = pl.ds(pl.multiple_of(c * chunk, chunk), chunk)
        spec = jnp.dot(
            halves[c // (chunks1 // 2)], table[:, columns], preferred_element_type=F32
        ).astype(BF)
        for k in range(per1):
            target = c * per1 + k
            send1[target] = spec[:, k * lanes : (k + 1) * lanes]

            @pl.when(target != me_t)
            def _():
                copy1(target, me_t).start()

        return carry

    lax.fori_loop(0, chunks1, spectrum_step, 0)
    own1 = pltpu.make_async_copy(send1.at[me_t], recv1.at[me_t], lsem.at[1])
    own1.start()
    split_positions(spot, row_ref, plane_id, hat.shape[1])
    fill_hat(hat, spot, False)
    own1.wait()

    def wait1(i, carry):
        other = lax.rem(me_t + i, count_trans)
        copy1(other, me_t).wait_send()
        copy1(me_t, other).wait_recv()
        return carry

    lax.fori_loop(1, count_trans, wait1, 0)

    columns = recv1[...].reshape(hat.shape[1], lanes)
    for c in range(half // chunk):
        low = jnp.dot(hat[c * chunk : (c + 1) * chunk, :], columns, preferred_element_type=F32)
        high = jnp.dot(
            hat[half + c * chunk : half + (c + 1) * chunk, :], columns,
            preferred_element_type=F32,
        )
        turned[0, :, c * chunk : (c + 1) * chunk] = (low + high).T.astype(BF)
        turned[1, :, c * chunk : (c + 1) * chunk] = (low - high).T.astype(BF)

    shape = (lanes, lanes)
    k2, lane_nyq, lane_sine, lane_end = fold_waves(
        length, width, me_t, lax.broadcasted_iota(jnp.int32, shape, 0)
    )
    lane_sign = jnp.where(lane_sine, 1.0, -1.0)
    scale2 = jnp.where(lane_end | lane_nyq, 1.0, 2.0) * (1.0 / length)
    inner = lax.broadcasted_iota(jnp.int32, shape, 1)
    for c in range(length // chunk):
        freq2 = jnp.dot(
            turned[c * chunk // half], table[:, c * chunk : (c + 1) * chunk],
            preferred_element_type=F32,
        )
        for k in range(chunk // lanes):
            block = c * (chunk // lanes) + k
            freq = freq2[:, k * lanes : (k + 1) * lanes]
            k1, row_nyq, row_sine, row_end = fold_waves(length, width, jnp.int32(block), inner)
            row_sign = jnp.where(row_sine, 1.0, -1.0)
            scale1 = jnp.where(row_end | row_nyq, 1.0, 2.0) * (1.0 / length)
            scale = scale1 * scale2 / jnp.maximum(k1 * k1 + k2 * k2, 1.0)
            d1 = (k1 * k1 - k2 * k2) * scale
            d2 = 2.0 * k1 * k2 * scale
            swap_rows = pltpu.roll(freq, width, 1)
            swap_lanes = jnp.concatenate([freq[width:], freq[:width]], axis=0)
            swap_both = pltpu.roll(swap_lanes, width, 1)
            first = d1 * freq
            extra = jnp.where(lane_nyq, row_sign * d2 * swap_rows, 0.0)
            second = jnp.where(lane_nyq, 0.0, -row_sign * lane_sign * d2 * swap_both)
            if block == 0:
                extra = jnp.where(
                    row_nyq, jnp.where(lane_nyq, 0.0, lane_sign * d2 * swap_lanes), extra
                )
                second = jnp.where(row_nyq, jnp.where(lane_nyq, d2 * freq, 0.0), second)
            where = slice(block * lanes, (block + 1) * lanes)
            fields[:lanes, where] = (first + extra).astype(BF)
            fields[lanes:, where] = second.astype(BF)

    def place(other):
        begin = pl.multiple_of((other // count_los) * lanes, lanes)
        return out_ref.at[lax.rem(other, count_los), :, :, pl.ds(begin, lanes)]

    def copy2(target, source):
        return pltpu.make_async_remote_copy(
            src_ref=send2.at[target], dst_ref=place(source),
            send_sem=ssem2.at[target], recv_sem=rsem2.at[source],
            device_id=(target // count_los, lax.rem(target, count_los)),
            device_id_type=pl.DeviceIdType.MESH,
        )

    contract = (((1,), (1,)), ((), ()))
    per = chunk // rows_out
    chunks2 = half // chunk

    def back_step(i, carry):
        c = lax.rem(me // per + chunks2 // 2 + i, chunks2)
        rows = pl.ds(pl.multiple_of(c * chunk, chunk), chunk)
        part_e = lax.dot_general(
            table[rows, :half], fields[:, :half], contract, preferred_element_type=F32
        )
        part_o = lax.dot_general(
            table[rows, half:], fields[:, half:], contract, preferred_element_type=F32
        )
        for offset, value in ((0, part_e + part_o), (devices // 2, part_e - part_o)):
            value = value.astype(BF)
            for k in range(per):
                target = offset + c * per + k
                for comp in range(2):
                    send2[target, comp] = value[
                        k * rows_out : (k + 1) * rows_out, comp * lanes : (comp + 1) * lanes
                    ]

                @pl.when(target != me)
                def _():
                    copy2(target, me).start()

        return carry

    lax.fori_loop(0, chunks2, back_step, 0)
    own2 = pltpu.make_async_copy(send2.at[me], place(me), lsem.at[2])
    own2.start()
    own2.wait()

    def wait2(i, carry):
        other = lax.rem(me + i, devices)
        copy2(other, me).wait_send()
        copy2(me, other).wait_recv()
        return carry

    lax.fori_loop(1, devices, wait2, 0)
    table_copy.wait()


def last_kernel(
    slot_ref, bin_ref, eff_ref, arrived_ref, table_ref, out_ref, whole, sems
):
    step = pl.program_id(0)
    planes, comps, rows, length = arrived_ref.shape
    half = length // 2
    bins = eff_ref.shape[0]
    chunk = table_ref.shape[0]
    contract = (((1,), (1,)), ((), ()))
    values = arrived_ref[...].reshape(planes * comps * rows, length)
    part_e = lax.dot_general(
        values[:, :half], table_ref[:, :half], contract, preferred_element_type=F32
    )
    part_o = lax.dot_general(
        values[:, half:], table_ref[:, half:], contract, preferred_element_type=F32
    )
    sides = (part_e + part_o, part_e - part_o)
    weights = []
    for b in range(bins):
        row = []
        for slot in range(planes):
            plane = slot_ref[slot]
            row.append(jnp.where(b >= bin_ref[plane], eff_ref[b, plane], 0.0))
        weights.append(row)

    def out_copy(at, side):
        columns = pl.ds(pl.multiple_of(side * half + at * chunk, chunk), chunk)
        return pltpu.make_async_copy(
            whole.at[:, :, :, columns], out_ref.at[:, :, :, columns], sems.at[at, side]
        )

    for side in range(2):
        columns = pl.ds(pl.multiple_of(side * half + step * chunk, chunk), chunk)
        for comp in range(comps):
            maps = [
                sides[side][(slot * comps + comp) * rows : (slot * comps + comp + 1) * rows]
                for slot in range(planes)
            ]
            for b in range(bins):
                total = weights[b][0] * maps[0]
                for slot in range(1, planes):
                    total = total + weights[b][slot] * maps[slot]
                whole[comp, b, :, columns] = total
        out_copy(step, side).start()

    @pl.when(step == half // chunk - 1)
    def _():
        for at in range(half // chunk):
            for side in range(2):
                out_copy(at, side).wait()


def body_kernel(density, row_pos, col_pos, plane_of_slot, plane_bin, efficiency):
    count_trans = lax.axis_size("trans")
    count_los = lax.axis_size("los")
    rows_in, cells = density.shape[1:]
    length = row_pos.shape[1]
    half = length // 2
    width = half // count_trans
    lanes = 2 * width
    bins = efficiency.shape[0]
    devices = count_trans * count_los
    rows_out = length // devices

    tables = [jnp.asarray(t) for t in small_tables(length, width)]
    vmem = pl.BlockSpec(memory_space=pltpu.VMEM)
    smem = pl.BlockSpec(memory_space=pltpu.SMEM)
    arrived, table = pl.pallas_call(
        functools.partial(middle_kernel, count_trans, count_los, length),
        out_shape=[
            jax.ShapeDtypeStruct((count_los, 2, rows_out, length), BF),
            jax.ShapeDtypeStruct((half, length), BF),
        ],
        in_specs=[smem] + [vmem] * 7,
        out_specs=[vmem, pl.BlockSpec(memory_space=pl.ANY)],
        scratch_shapes=[
            pltpu.VMEM((half, length), BF),
            pltpu.VMEM((length, cells), BF),
            pltpu.VMEM((2, rows_in, half), BF),
            pltpu.VMEM((count_trans, rows_in, lanes), BF),
            pltpu.VMEM((count_trans, rows_in, lanes), BF),
            pltpu.VMEM((2, lanes, half), BF),
            pltpu.VMEM((2 * lanes, length), BF),
            pltpu.VMEM((devices, 2, rows_out, lanes), BF),
            pltpu.VMEM((8, length), F32),
            pltpu.SemaphoreType.DMA((count_trans,)),
            pltpu.SemaphoreType.DMA((count_trans,)),
            pltpu.SemaphoreType.DMA((devices,)),
            pltpu.SemaphoreType.DMA((devices,)),
            pltpu.SemaphoreType.DMA((3,)),
        ],
        compiler_params=pltpu.CompilerParams(
            collective_id=0, has_side_effects=True, vmem_limit_bytes=56 * 1024 * 1024
        ),
    )(plane_of_slot, density[0], row_pos, col_pos, *tables)
    chunk = 256
    return pl.pallas_call(
        last_kernel,
        grid=(half // chunk,),
        out_shape=jax.ShapeDtypeStruct((2, bins, rows_out, length), F32),
        in_specs=[smem] * 3
        + [
            pl.BlockSpec((count_los, 2, rows_out, length), lambda i: (0, 0, 0, 0)),
            pl.BlockSpec((chunk, length), lambda i: (i, 0)),
        ],
        out_specs=pl.BlockSpec(memory_space=pl.ANY),
        scratch_shapes=[
            pltpu.VMEM((2, bins, rows_out, length), F32),
            pltpu.SemaphoreType.DMA((half // chunk, 2)),
        ],
        compiler_params=pltpu.CompilerParams(vmem_limit_bytes=32 * 1024 * 1024),
    )(plane_of_slot, plane_bin, efficiency, arrived, table)


def body(density, row_pos, *rest):
    length = row_pos.shape[1]
    fits = length // lax.axis_size("trans") == 128 and density.shape[1] == 128
    fits = fits and length % 512 == 0 and density.shape[2] == length
    return (body_kernel if fits else body_plain)(density, row_pos, *rest)


def solution(mesh):
    placed = (P("los", "trans", None), P(), P(), P(), P(), P())
    return jax.shard_map(
        body,
        mesh=mesh,
        in_specs=placed,
        out_specs=P(None, None, ("trans", "los"), None),
        check_vma=False,
    )
```

```python
import functools

import jax
import jax.numpy as jnp
import numpy as np
from jax import lax
from jax.experimental import pallas as pl
from jax.experimental.pallas import tpu as pltpu
from jax.sharding import PartitionSpec as P

BF = jnp.bfloat16
F32 = jnp.float32
STEP = 32


def slot_layout(length, width):
    half = length // 2
    blocks = half // width
    block = np.arange(2 * half) // (2 * width)
    inner = np.arange(2 * half) % (2 * width)
    is_sine = inner >= width
    member = inner % width
    odd = block >= blocks // 2
    wave = 2 * (np.where(odd, block - blocks // 2, block) * width + member) + odd
    nyquist = is_sine & (wave == 0)
    wave = np.where(nyquist, half, wave)
    phase = np.where(is_sine & ~nyquist, 0.5 * np.pi, 0.0)
    return wave, phase


def small_tables(length, width):
    half = length // 2
    wave, phase = slot_layout(length, width)
    coarse = (np.arange(half // STEP)[:, None] * STEP * wave[None, :]) % length
    fine = (np.arange(STEP)[:, None] * wave[None, :]) % length
    coarse = coarse * (2 * np.pi / length)
    fine = fine * (2 * np.pi / length) + phase[None, :]
    return [np.float32(t) for t in (np.cos(coarse), np.sin(coarse), np.cos(fine), np.sin(fine))]


def full_table(length, width):
    half = length // 2
    cos_a, sin_a, cos_b, sin_b = [jnp.asarray(t) for t in small_tables(length, width)]
    table = cos_a[:, None] * cos_b[None] - sin_a[:, None] * sin_b[None]
    table = table.reshape(half, 2 * half).astype(BF)
    return table[:, :half], table[:, half:]


def hat_rows(positions, cells):
    base = jnp.floor(positions)
    frac = positions - base
    low = base.astype(jnp.int32) % cells
    high = (low + 1) % cells
    index = jnp.arange(cells, dtype=jnp.int32)[None, :]
    value = jnp.where(index == low[:, None], (1.0 - frac)[:, None], 0.0)
    return jnp.where(index == high[:, None], frac[:, None], value).astype(BF)


def dot(a, b, dims):
    return lax.dot_general(a, b, (dims, ((), ())), preferred_element_type=F32)


def lane_waves(length, width, index):
    blocks = length // 2 // width
    lane = lax.broadcasted_iota(jnp.int32, (1, 2 * width), 1)
    is_sine = lane >= width
    member = jnp.where(is_sine, lane - width, lane)
    odd = (index >= blocks // 2).astype(jnp.int32)
    wave = 2 * ((index - odd * (blocks // 2)) * width + member) + odd
    special = is_sine & (wave == 0)
    wave = jnp.where(special, -(length // 2), wave)
    return wave.astype(F32), special, is_sine


def body_plain(density, row_pos, col_pos, plane_of_slot, plane_bin, efficiency):
    count_trans = lax.axis_size("trans")
    count_los = lax.axis_size("los")
    cells = density.shape[2]
    length = row_pos.shape[1]
    half = length // 2
    width = half // count_trans
    planes = row_pos.shape[0]
    bins = efficiency.shape[0]
    rows_out = length // (count_trans * count_los)
    plane_id = plane_of_slot[lax.axis_index("los")]
    even, odd = full_table(length, width)

    cols_hat = hat_rows(col_pos[plane_id], cells)
    sampled = dot(density[0], cols_hat, ((1,), (1,)))
    plus = (sampled[:, :half] + sampled[:, half:]).astype(BF)
    minus = (sampled[:, :half] - sampled[:, half:]).astype(BF)
    spec = jnp.concatenate([dot(plus, even, ((1,), (0,))), dot(minus, odd, ((1,), (0,)))], axis=1).astype(BF)
    columns = lax.all_to_all(spec, "trans", split_axis=1, concat_axis=0, tiled=True)

    rows_hat = hat_rows(row_pos[plane_id], cells)
    mapped = dot(rows_hat, columns, ((1,), (0,)))
    plus = (mapped[:half] + mapped[half:]).astype(BF)
    minus = (mapped[:half] - mapped[half:]).astype(BF)
    freq = jnp.concatenate([dot(even, plus, ((0,), (0,))), dot(odd, minus, ((0,), (0,)))], axis=0)
    wave_np, phase_np = slot_layout(length, width)
    nyq_np = wave_np == half
    k1 = jnp.asarray(np.where(nyq_np, -half, wave_np), F32)[:, None]
    row_nyq = jnp.asarray(nyq_np)[:, None]
    row_sign = jnp.asarray(np.where(phase_np > 0, 1.0, -1.0), F32)[:, None]
    k2, lane_nyq, lane_sine = lane_waves(length, width, lax.axis_index("trans"))
    lane_sign = jnp.where(lane_sine, 1.0, -1.0)
    square = jnp.maximum(k1 * k1 + k2 * k2, 1.0)
    scale1 = jnp.asarray(np.where((wave_np == 0) | nyq_np, 1.0, 2.0) / length, F32)[:, None]
    scale2 = jnp.where((k2 == 0.0) | lane_nyq, 1.0, 2.0) / length
    scale = scale1 * scale2 / square
    d1 = (k1 * k1 - k2 * k2) * scale
    d2 = 2.0 * k1 * k2 * scale
    grid = freq.reshape(-1, 2, width, 2 * width)
    swap_rows = jnp.flip(grid, 1).reshape(freq.shape)
    swap_lanes = jnp.roll(freq, width, axis=1)
    swap_both = jnp.roll(swap_rows, width, axis=1)
    first = d1 * freq
    first = first + jnp.where(lane_nyq & ~row_nyq, row_sign * d2 * swap_rows, 0.0)
    first = first + jnp.where(row_nyq & ~lane_nyq, lane_sign * d2 * swap_lanes, 0.0)
    second = jnp.where(
        row_nyq,
        jnp.where(lane_nyq, d2 * freq, 0.0),
        jnp.where(lane_nyq, 0.0, -row_sign * lane_sign * d2 * swap_both),
    )
    fields = jnp.concatenate([first, second], axis=1).astype(BF)
    part_e = dot(even, fields[:half], ((1,), (0,)))
    part_o = dot(odd, fields[half:], ((1,), (0,)))
    back = jnp.concatenate([part_e + part_o, part_e - part_o], axis=0).astype(BF)

    back = back.reshape(count_trans * count_los, rows_out, 2, 2 * width)
    arrived = lax.all_to_all(back, ("trans", "los"), split_axis=0, concat_axis=0, tiled=True)
    arrived = arrived.reshape(count_trans, count_los, rows_out, 2, 2 * width).transpose(1, 3, 2, 0, 4)
    arrived = arrived.reshape(count_los * 2 * rows_out, length)
    part_e = dot(arrived[:, :half], even, ((1,), (1,)))
    part_o = dot(arrived[:, half:], odd, ((1,), (1,)))
    maps = jnp.concatenate([part_e + part_o, part_e - part_o], axis=1)
    maps = maps.reshape(count_los, 2, rows_out, length)
    slot_eff = efficiency[:, plane_of_slot]
    behind = jnp.arange(bins)[:, None] >= plane_bin[plane_of_slot][None, :]
    weights = jnp.where(behind, slot_eff, 0.0)
    total = 0.0
    for slot in range(planes):
        total = total + weights[None, :, slot, None, None] * maps[slot][:, None]
    return total


def fold_waves(length, width, block, inner):
    blocks = length // 2 // width
    is_sine = inner >= width
    member = jnp.where(is_sine, inner - width, inner)
    odd = (block >= blocks // 2).astype(jnp.int32)
    wave = 2 * ((block - odd * (blocks // 2)) * width + member) + odd
    nyquist = is_sine & (wave == 0)
    ends = (wave == 0) & ((block == 0) | ~is_sine)
    wave = jnp.where(nyquist, -(length // 2), wave)
    return wave.astype(F32), nyquist, is_sine, ends


def split_positions(spot, pos_ref, plane_id, cells):
    here = pos_ref[0:1, :]
    for plane in range(1, pos_ref.shape[0]):
        here = jnp.where(plane_id == plane, pos_ref[plane : plane + 1, :], here)
    base = jnp.floor(here)
    low = jnp.where(base >= cells, base - cells, base)
    spot[0:1, :] = low
    spot[1:2, :] = jnp.where(low == cells - 1, 0.0, low + 1.0)
    spot[2:3, :] = here - base


def fill_hat(out_ref, spot, positions_on_lanes):
    cells = out_ref.shape[0]
    part = 128

    def step(i, carry):
        rows = pl.ds(pl.multiple_of(i * part, part), part)
        if not positions_on_lanes:
            low, high, frac = [
                jnp.broadcast_to(spot[k : k + 1, rows], (part, part)).T for k in range(3)
            ]
            less = 1.0 - frac
        for j in range(out_ref.shape[1] // part):
            columns = slice(j * part, (j + 1) * part)
            if positions_on_lanes:
                low, high, frac = [spot[k : k + 1, columns] for k in range(3)]
                less = 1.0 - frac
                index = lax.broadcasted_iota(jnp.int32, (part, part), 0) + i * part
            else:
                lane = lax.broadcasted_iota(jnp.int32, (part, part), 1)
                count = out_ref.shape[1] // part // 2
                start = 2 * (j % count) * part + (part // 2) * (j // count)
                index = lane + jnp.where(lane >= part // 2, part // 2, 0) + start
            index = index.astype(F32)
            value = jnp.where(index == high, frac, 0.0)
            value = jnp.where(index == low, less, value)
            out_ref[rows, columns] = value.astype(BF)
        return carry

    lax.fori_loop(0, cells // part, step, 0)


def middle_kernel(
    count_trans, count_los, length,
    slot_ref, row_ref, col_ref, dens_hbm, *refs
):
    small_hbm, refs = refs[:4], refs[4:]
    out_ref, table, hat, halves, send1, recv1, turned, fields, send2 = refs[:9]
    spot, dens_ref, cos_a, sin_a, cos_b, sin_b, ssem1, rsem1, ssem2, rsem2, lsem = refs[9:]
    loads = [
        pltpu.make_async_copy(source, target, lsem.at[3 + k])
        for k, (source, target) in enumerate(
            zip((dens_hbm, *small_hbm), (dens_ref, cos_a, sin_a, cos_b, sin_b))
        )
    ]
    for load in loads:
        load.start()
    me_t = lax.axis_index("trans")
    me_l = lax.axis_index("los")
    devices = count_trans * count_los
    me = me_t * count_los + me_l
    half = length // 2
    width = half // count_trans // 2
    lanes = 2 * width
    rows_out = length // devices
    chunk = 256
    barrier = pltpu.get_barrier_semaphore()

    def greet(i, carry):
        other = lax.rem(me + i, devices)
        pl.semaphore_signal(
            barrier, inc=1,
            device_id=(other // count_los, lax.rem(other, count_los)),
            device_id_type=pl.DeviceIdType.MESH,
        )
        return carry

    lax.fori_loop(1, devices, greet, 0)

    plane_id = slot_ref[me_l]
    split_positions(spot, col_ref, plane_id, hat.shape[0])
    fill_hat(hat, spot, True)
    for load in loads:
        load.wait()

    def table_step(i, carry):
        rows = pl.ds(pl.multiple_of(i * STEP, STEP), STEP)
        value = cos_a[pl.ds(i, 1), :] * cos_b[...] - sin_a[pl.ds(i, 1), :] * sin_b[...]
        table[rows, :] = value.astype(BF)
        return carry

    lax.fori_loop(0, half // STEP, table_step, 0)

    for c in range(half // chunk):
        low = jnp.dot(dens_ref[...], hat[:, c * chunk : (c + 1) * chunk], preferred_element_type=F32)
        high = jnp.dot(
            dens_ref[...], hat[:, half + c * chunk : half + (c + 1) * chunk],
            preferred_element_type=F32,
        )
        halves[0, :, c * chunk : (c + 1) * chunk] = (low + high).astype(BF)
        halves[1, :, c * chunk : (c + 1) * chunk] = (low - high).astype(BF)
    def copy1(parity, target, source):
        return pltpu.make_async_remote_copy(
            src_ref=send1.at[parity, target], dst_ref=recv1.at[parity, source],
            send_sem=ssem1.at[parity, target], recv_sem=rsem1.at[parity, source],
            device_id=(target, me_l), device_id_type=pl.DeviceIdType.MESH,
        )

    pl.semaphore_wait(barrier, devices - 1)
    chunks1 = half // chunk
    per1 = chunk // lanes
    rows_half = send1.shape[2]
    owns = []
    for parity in range(2):

        def spectrum_step(i, carry):
            c = lax.rem(me_t // per1 + chunks1 // 2 + i, chunks1)
            columns = pl.ds(pl.multiple_of(parity * half + c * chunk, chunk), chunk)
            spec = jnp.dot(halves[parity], table[:, columns], preferred_element_type=F32)
            for k in range(per1):
                target = c * per1 + k
                block = spec[:, k * lanes : (k + 1) * lanes]
                send1[parity, target] = jnp.concatenate(
                    [block[:rows_half], block[rows_half:]], axis=1
                ).astype(BF)

                @pl.when(target != me_t)
                def _():
                    copy1(parity, target, me_t).start()

            return carry

        lax.fori_loop(0, chunks1, spectrum_step, 0)
        owns.append(
            pltpu.make_async_copy(
                send1.at[parity, me_t], recv1.at[parity, me_t], lsem.at[parity]
            )
        )
        owns[parity].start()
    split_positions(spot, row_ref, plane_id, hat.shape[1])
    fill_hat(hat, spot, False)

    def place(parity, other):
        begin = pl.multiple_of((other // count_los) * 2 * lanes, 2 * lanes)
        return out_ref.at[parity, lax.rem(other, count_los), :, pl.ds(begin, 2 * lanes)]

    def copy2(parity, target, source):
        return pltpu.make_async_remote_copy(
            src_ref=send2.at[parity, target], dst_ref=place(parity, source),
            send_sem=ssem2.at[parity, target], recv_sem=rsem2.at[parity, source],
            device_id=(target // count_los, lax.rem(target, count_los)),
            device_id_type=pl.DeviceIdType.MESH,
        )

    contract = (((1,), (1,)), ((), ()))
    per = chunk // rows_out
    chunks2 = half // chunk
    shape = (lanes, chunk)
    inner = lax.broadcasted_iota(jnp.int32, shape, 1)
    member = jnp.bitwise_and(inner, lanes - 1)
    for parity in range(2):
        owns[parity].wait()

        def wait1(i, carry):
            other = lax.rem(me_t + i, count_trans)
            copy1(parity, other, me_t).wait_send()
            copy1(parity, me_t, other).wait_recv()
            return carry

        lax.fori_loop(1, count_trans, wait1, 0)
        columns = recv1[parity].reshape(half, 2 * lanes)

        def resample(begin):
            rows = slice(begin, begin + chunk)
            one = jnp.dot(hat[rows, :half], columns, preferred_element_type=F32)
            two = jnp.dot(hat[rows, half:], columns, preferred_element_type=F32)
            return one + pltpu.roll(two, lanes, 1)

        for c in range(half // chunk):
            low = resample(c * chunk)
            high = resample(half + c * chunk)
            turned[0, :, c * chunk : (c + 1) * chunk] = (low + high).T[:lanes].astype(BF)
            turned[1, :, c * chunk : (c + 1) * chunk] = (low - high).T[:lanes].astype(BF)

        k2, lane_nyq, lane_sine, lane_end = fold_waves(
            length, width, parity * count_trans + me_t,
            lax.broadcasted_iota(jnp.int32, shape, 0),
        )
        lane_sign = jnp.where(lane_sine, 1.0, -1.0)
        scale2 = jnp.where(lane_end | lane_nyq, 1.0, 2.0) * (1.0 / length)

        def swap(value):
            ahead = pltpu.roll(value, chunk - width, 1)
            return jnp.where(member < width, ahead, pltpu.roll(value, width, 1))

        for c in range(length // chunk):
            where = slice(c * chunk, (c + 1) * chunk)
            freq = jnp.dot(
                turned[c // chunks2], table[:, where], preferred_element_type=F32
            )
            block = c * (chunk // lanes) + lax.div(inner, lanes)
            k1, row_nyq, row_sine, row_end = fold_waves(length, width, block, member)
            row_sign = jnp.where(row_sine, 1.0, -1.0)
            scale1 = jnp.where(row_end | row_nyq, 1.0, 2.0) * (1.0 / length)
            scale = scale1 * scale2 / jnp.maximum(k1 * k1 + k2 * k2, 1.0)
            d1 = (k1 * k1 - k2 * k2) * scale
            d2 = 2.0 * k1 * k2 * scale
            swap_lanes = jnp.concatenate([freq[width:], freq[:width]], axis=0)
            swap_both = swap(swap_lanes)
            first = d1 * freq
            second = -row_sign * lane_sign * d2 * swap_both
            if parity == 0:
                extra = jnp.where(lane_nyq, row_sign * d2 * swap(freq), 0.0)
                second = jnp.where(lane_nyq, 0.0, second)
            else:
                extra = jnp.zeros_like(freq)
            if c == 0:
                extra = jnp.where(
                    row_nyq, jnp.where(lane_nyq, 0.0, lane_sign * d2 * swap_lanes), extra
                )
                second = jnp.where(row_nyq, jnp.where(lane_nyq, d2 * freq, 0.0), second)
            fields[:lanes, where] = (first + extra).astype(BF)
            fields[lanes:, where] = second.astype(BF)

        def back_step(i, carry):
            c = lax.rem(me // per + chunks2 // 2 + i, chunks2)
            rows = pl.ds(pl.multiple_of(c * chunk, chunk), chunk)
            part_e = lax.dot_general(
                table[rows, :half], fields[:, :half], contract, preferred_element_type=F32
            )
            part_o = lax.dot_general(
                table[rows, half:], fields[:, half:], contract, preferred_element_type=F32
            )
            for offset, value in ((0, part_e + part_o), (devices // 2, part_e - part_o)):
                value = value.astype(BF)
                for k in range(per):
                    target = offset + c * per + k
                    send2[parity, target] = value[k * rows_out : (k + 1) * rows_out]

                    @pl.when(target != me)
                    def _():
                        copy2(parity, target, me).start()

            return carry

        lax.fori_loop(0, chunks2, back_step, 0)
        own2 = pltpu.make_async_copy(send2.at[parity, me], place(parity, me), lsem.at[2])
        own2.start()
        own2.wait()

    for parity in range(2):

        def wait2(i, carry):
            other = lax.rem(me + i, devices)
            copy2(parity, other, me).wait_send()
            copy2(parity, me, other).wait_recv()
            return carry

        lax.fori_loop(1, devices, wait2, 0)


def last_kernel(
    slot_ref, bin_ref, eff_ref, arrived_ref, cos_a, sin_a, cos_b, sin_b, out_ref,
    whole, values, table, sems,
):
    step = pl.program_id(0)
    comps = 2
    planes, rows, length = arrived_ref.shape[1:]
    half = length // 2
    bins = eff_ref.shape[1]
    chunk = table.shape[0]
    contract = (((1,), (1,)), ((), ()))

    @pl.when(step == 0)
    def _():
        tile = 128
        first = lax.broadcasted_iota(jnp.int32, (rows, tile), 1) < tile // 2
        for parity in range(2):
            for slot in range(planes):
                for pair in range(half // tile):
                    left, right = [
                        arrived_ref[
                            parity, slot, :, (2 * pair + k) * tile : (2 * pair + k + 1) * tile
                        ].astype(F32)
                        for k in range(2)
                    ]
                    zero = jnp.where(first, left, pltpu.roll(right, tile // 2, 1))
                    one = jnp.where(first, pltpu.roll(left, tile // 2, 1), right)
                    for comp, value in enumerate((zero, one)):
                        begin = (slot * comps + comp) * rows
                        values[
                            parity, begin : begin + rows, pair * tile : (pair + 1) * tile
                        ] = value.astype(BF)

    for k in range(chunk // STEP):
        at = step * (chunk // STEP) + k
        value = cos_a[pl.ds(at, 1), :] * cos_b[...] - sin_a[pl.ds(at, 1), :] * sin_b[...]
        table[k * STEP : (k + 1) * STEP, :] = value.astype(BF)
    part_e = lax.dot_general(
        values[0], table[:, :half], contract, preferred_element_type=F32
    )
    part_o = lax.dot_general(
        values[1], table[:, half:], contract, preferred_element_type=F32
    )
    sides = (part_e + part_o, part_e - part_o)
    weights = []
    for b in range(bins):
        row = []
        for slot in range(planes):
            plane = slot_ref[slot]
            row.append(jnp.where(b >= bin_ref[plane], eff_ref[plane, b], 0.0))
        weights.append(row)

    def out_copy(at, side):
        columns = pl.ds(pl.multiple_of(side * half + at * chunk, chunk), chunk)
        return pltpu.make_async_copy(
            whole.at[:, :, :, columns], out_ref.at[:, :, :, columns], sems.at[at, side]
        )

    for side in range(2):
        columns = pl.ds(pl.multiple_of(side * half + step * chunk, chunk), chunk)
        for comp in range(comps):
            maps = [
                sides[side][(slot * comps + comp) * rows : (slot * comps + comp + 1) * rows]
                for slot in range(planes)
            ]
            for b in range(bins):
                total = weights[b][0] * maps[0]
                for slot in range(1, planes):
                    total = total + weights[b][slot] * maps[slot]
                whole[comp, b, :, columns] = total
        out_copy(step, side).start()

    @pl.when(step == half // chunk - 1)
    def _():
        for at in range(half // chunk):
            for side in range(2):
                out_copy(at, side).wait()


def body_kernel(density, row_pos, col_pos, plane_of_slot, plane_bin, efficiency):
    count_trans = lax.axis_size("trans")
    count_los = lax.axis_size("los")
    rows_in, cells = density.shape[1:]
    length = row_pos.shape[1]
    half = length // 2
    width = half // count_trans // 2
    lanes = 2 * width
    bins = efficiency.shape[0]
    devices = count_trans * count_los
    rows_out = length // devices

    tables = [jnp.asarray(t) for t in small_tables(length, width)]
    vmem = pl.BlockSpec(memory_space=pltpu.VMEM)
    smem = pl.BlockSpec(memory_space=pltpu.SMEM)
    arrived = pl.pallas_call(
        functools.partial(middle_kernel, count_trans, count_los, length),
        out_shape=jax.ShapeDtypeStruct((2, count_los, rows_out, 2 * lanes * count_trans), BF),
        in_specs=[smem] + [vmem] * 2 + [pl.BlockSpec(memory_space=pltpu.HBM)] * 5,
        out_specs=vmem,
        scratch_shapes=[
            pltpu.VMEM((half, length), BF),
            pltpu.VMEM((length, cells), BF),
            pltpu.VMEM((2, rows_in, half), BF),
            pltpu.VMEM((2, count_trans, rows_in // 2, 2 * lanes), BF),
            pltpu.VMEM((2, count_trans, rows_in // 2, 2 * lanes), BF),
            pltpu.VMEM((2, lanes, half), BF),
            pltpu.VMEM((2 * lanes, length), BF),
            pltpu.VMEM((2, devices, rows_out, 2 * lanes), BF),
            pltpu.VMEM((8, length), F32),
            pltpu.VMEM((rows_in, cells), BF),
            *[pltpu.VMEM(t.shape, F32) for t in tables],
            pltpu.SemaphoreType.DMA((2, count_trans)),
            pltpu.SemaphoreType.DMA((2, count_trans)),
            pltpu.SemaphoreType.DMA((2, devices)),
            pltpu.SemaphoreType.DMA((2, devices)),
            pltpu.SemaphoreType.DMA((8,)),
        ],
        compiler_params=pltpu.CompilerParams(
            collective_id=0, has_side_effects=True, vmem_limit_bytes=63 * 1024 * 1024
        ),
    )(plane_of_slot, row_pos, col_pos, density[0], *tables)
    chunk = 256
    return pl.pallas_call(
        last_kernel,
        grid=(half // chunk,),
        out_shape=jax.ShapeDtypeStruct((2, bins, rows_out, length), F32),
        in_specs=[smem] * 3
        + [
            pl.BlockSpec(arrived.shape, lambda i: (0, 0, 0, 0)),
            *[pl.BlockSpec(t.shape, lambda i: (0, 0)) for t in tables],
        ],
        out_specs=pl.BlockSpec(memory_space=pl.ANY),
        scratch_shapes=[
            pltpu.VMEM((2, bins, rows_out, length), F32),
            pltpu.VMEM((2, count_los * 2 * rows_out, half), BF),
            pltpu.VMEM((chunk, length), BF),
            pltpu.SemaphoreType.DMA((half // chunk, 2)),
        ],
        compiler_params=pltpu.CompilerParams(vmem_limit_bytes=63 * 1024 * 1024),
    )(plane_of_slot, plane_bin, efficiency.T, arrived, *tables)


def body(density, row_pos, *rest):
    length = row_pos.shape[1]
    fits = length // lax.axis_size("trans") == 128 and density.shape[1] == 128
    fits = fits and length % 512 == 0 and density.shape[2] == length
    return (body_kernel if fits else body_plain)(density, row_pos, *rest)


def solution(mesh):
    placed = (P("los", "trans", None), P(), P(), P(), P(), P())
    return jax.shard_map(
        body,
        mesh=mesh,
        in_specs=placed,
        out_specs=P(None, None, ("trans", "los"), None),
        check_vma=False,
    )
```
